32 devices in a mesh: groups: 2 (over x), pb: 16 (over z, y, core).
Axes of the slice: x: 2, y: 2, z: 4, core: 2. Of those that a mesh axis runs over, the one named last changes fastest.
Arguments:
- tokens: bfloat16 [6144, 512], P(('groups', 'pb')), parts along dimension 0, may hold values from -6 to 6
- stamps: int32 [6144], P(('groups', 'pb')), parts along dimension 0, may hold values from 0 to 1086324736, as said below
- norm_gain: float32 [512], replicated, may hold values from 0.5 to 1.5
- w_proj: bfloat16 [512, 2048], replicated, may hold values from -0.25 to 0.25
- rel_bias: float32 [8, 16], replicated, may hold values from -1.5 to 1.5
- attn_gain: float32 [512], replicated, may hold values from 0.5 to 1.5
- w_out: bfloat16 [512, 512], replicated, may hold values from -0.25 to 0.25
Outputs:
- mixed: bfloat16 [6144, 512], P(('groups', 'pb')), parts along dimension 0
The draws below stay inside these ranges and needn't reach their ends.
There are 2 independent parts, one for each index of `groups`. The reference program is written for one: setup_inputs(seed, part) draws one part's arguments, and reference() takes and returns one part's arrays. A program takes and returns all parts, laid end to end along the dimension named above; an argument that names none is the same for every part. Nothing has to cross between parts.
Inputs may be any that keep to these rules, and one draw needn't show every extreme that they name: `stamps`: stamps never fall from one row to the next.
All inputs are finite; a program needn't handle non-finite values.
Results may differ from the reference program's by a relative error of at most 0.008.
Values may be sent and summed in bfloat16 or wider, within the bound.
A program may use at most 128 MiB of HBM per device.

```python
import jax
import jax.numpy as jnp
from jax import lax

D = 512
HEADS = 8
HEAD = 64
BUCKETS = 16
TOK_DEV = 192
TOKENS = 3072


def draw_stamps(key, part):
    first_key = jax.random.fold_in(key, 11)
    second_key = jax.random.fold_in(key, 12)
    third_key = jax.random.fold_in(key, 13)
    exponent = jax.random.randint(first_key, (TOKENS,), 0, 13)
    chosen = jax.random.permutation(third_key, TOKENS)[:16]
    jump_bits = jnp.zeros((TOKENS,), jnp.int32).at[chosen].set(13 + jnp.arange(16, dtype=jnp.int32))
    jump_mask = jump_bits > 0
    exponent = jnp.where(jump_mask, jump_bits, exponent)
    ones_row = jnp.ones((TOKENS,), jnp.int32)
    low_end = jnp.where(jump_mask, jnp.left_shift(ones_row, exponent), 0)
    high_end = jnp.where(jump_mask, jnp.left_shift(ones_row, exponent + 1), jnp.left_shift(ones_row, exponent) + 1)
    spacing = jax.random.randint(second_key, (TOKENS,), low_end, high_end)
    running = jnp.cumsum(spacing).astype(jnp.int32)
    top_value = jnp.int32(4096 * TOKENS + 2 ** 30)
    return (running + (top_value - running[-1])).astype(jnp.int32)


def block_scale(key, extent, cuts, low, high):
    def one(position, blocks):
        draws = jax.random.uniform(jax.random.fold_in(jax.random.fold_in(key, 6), position), (blocks,), jnp.float32, low / len(cuts), high / len(cuts))
        return jnp.repeat(jnp.exp(draws), extent[position] // blocks).reshape((-1,) + (1,) * (len(extent) - position - 1))

    level = one(*cuts[0])
    for cut in cuts[1:]:
        level = level * one(*cut)
    return level


def gaussian(own_key, dims, scale, bound, cuts=(), kind=jnp.bfloat16):
    values = jax.random.normal(own_key, dims, jnp.float32) * scale
    if len(cuts) > 0:
        values = block_scale(own_key, dims, cuts, -0.22, 0.18) * values
    return jnp.clip(values, min=-bound, max=bound).astype(kind)


def setup_inputs(seed: int = 0, part: int = 0) -> dict:
    key_of = jax.random.split(jax.random.key(seed), 8)
    part_splits = jax.random.split(jax.random.fold_in(key_of[7], part), 8)
    return {
        "tokens": gaussian(part_splits[0], (TOKENS, D), 1.0, 6.0, ((0, 16),)),
        "stamps": draw_stamps(jax.random.fold_in(jax.random.fold_in(key_of[7], part), 71), part),
        "norm_gain": jnp.clip(1.0 + 0.1 * jax.random.normal(key_of[2], (D,), jnp.float32), 0.5, 1.5),
        "w_proj": gaussian(key_of[3], (D, 4 * D), D ** -0.5, 0.25),
        "rel_bias": jnp.clip(jax.random.uniform(key_of[4], (HEADS, BUCKETS), jnp.float32, -1.5, 1.5), -1.5, 1.5),
        "attn_gain": jnp.clip(1.0 + 0.1 * jax.random.normal(key_of[5], (D,), jnp.float32), 0.5, 1.5),
        "w_out": gaussian(key_of[6], (D, D), D ** -0.5, 0.25),
    }


epsilon = 1e-05

def layer_norm(values, gain):
    centered = values - lax.optimization_barrier(jnp.mean(values, axis=-1, keepdims=True))
    spread = lax.optimization_barrier(jnp.mean(centered * centered, axis=-1, keepdims=True))
    return centered * lax.rsqrt(spread + epsilon) * gain

def bucket_of(elapsed):
    bucket_ids = jnp.zeros(elapsed.shape, jnp.int32)
    for exponent in range(BUCKETS - 1):
        bucket_ids = bucket_ids + (elapsed >= 4 ** exponent).astype(jnp.int32)
    return bucket_ids

def reference(tokens, stamps, norm_gain, w_proj, rel_bias, attn_gain, w_out):
    normed = layer_norm(tokens.astype(jnp.float32), norm_gain).astype(jnp.bfloat16)
    projected = jnp.dot(normed, w_proj, preferred_element_type=jnp.float32)
    gate_vals = jax.nn.silu(projected[:, :D]).astype(jnp.bfloat16)
    queries = projected[:, D:2 * D].astype(jnp.bfloat16)
    key_rows = projected[:, 2 * D:3 * D].astype(jnp.bfloat16)
    value_rows = projected[:, 3 * D:].astype(jnp.bfloat16)
    q_heads = queries.astype(jnp.float32).reshape(TOKENS, HEADS, HEAD)
    k_heads = key_rows.astype(jnp.float32).reshape(TOKENS, HEADS, HEAD)
    v_heads = value_rows.astype(jnp.float32).reshape(TOKENS, HEADS, HEAD)
    positions = jnp.arange(TOKENS, dtype=jnp.int32)

    def one_block(start):
        q_block = lax.dynamic_slice_in_dim(q_heads, start, TOK_DEV, 0)
        q_pos = start + jnp.arange(TOK_DEV, dtype=jnp.int32)
        q_stamp = lax.dynamic_slice_in_dim(stamps, start, TOK_DEV, 0)
        scores = jnp.einsum('qhd,khd->hqk', q_block, k_heads) * HEAD ** (-0.5)
        bucket = bucket_of(q_stamp[:, None] - stamps[None, :])
        scores = scores + rel_bias[:, bucket]
        visible = positions[None, :] <= q_pos[:, None]
        weight = jnp.where(visible[None], jax.nn.silu(scores), 0.0).astype(jnp.bfloat16)
        mixture = jnp.einsum('hqk,khd->qhd', weight.astype(jnp.float32), v_heads)
        return mixture.reshape(TOK_DEV, D)
    block_starts = jnp.arange(0, TOKENS, TOK_DEV, dtype=jnp.int32)
    attended = lax.map(one_block, block_starts).reshape(TOKENS, D)
    gated = (layer_norm(attended, attn_gain) * gate_vals.astype(jnp.float32)).astype(jnp.bfloat16)
    result = tokens.astype(jnp.float32) + jnp.dot(gated, w_out, preferred_element_type=jnp.float32)
    return result.astype(jnp.bfloat16)
```

```python
import functools

import jax
import jax.numpy as jnp
from jax import lax
from jax.experimental import pallas as pl
from jax.experimental.pallas import tpu as pltpu
from jax.sharding import PartitionSpec as P

EPSILON = 1e-05
LANES = 128


def layer_norm(values, gain):
    centered = values - jnp.mean(values, axis=-1, keepdims=True)
    spread = jnp.mean(centered * centered, axis=-1, keepdims=True)
    return centered * lax.rsqrt(spread + EPSILON) * gain


def kernel(
    parts,
    heads,
    tokens_ref,
    stamps_ref,
    norm_gain_ref,
    w_proj_ref,
    bias_ref,
    attn_gain_ref,
    w_out_ref,
    out_ref,
    send_buf,
    kvq,
    stamp_all,
    stamp_keys,
    gate_buf,
    back_buf,
    att_buf,
    send_sem,
    fwd_sem,
    kv_sem,
    stamp_send_sem,
    stamp_sem,
    back_sem,
    att_sem,
):
    rows, width = tokens_ref.shape
    half = rows // 2
    head_size = width // heads
    splits = parts // heads
    slots = parts // splits
    blocks_per_tile = max(1, 384 // rows)
    key_tile = blocks_per_tile * rows
    buckets = bias_ref.shape[1]

    me = lax.axis_index("pb")
    my_head = me // splits
    my_split = me % splits

    def split_of(block):
        place = block % splits
        odd = (block // splits) % 2
        return place + odd * (splits - 1 - 2 * place)

    def block_of(slot, split):
        odd = slot % 2
        return slot * splits + split + odd * (splits - 1 - 2 * split)

    barrier = pltpu.get_barrier_semaphore()

    def greet(step, carry):
        other = lax.rem(me + step, parts)
        pl.semaphore_signal(
            barrier, inc=1, device_id={"pb": other}, device_id_type=pl.DeviceIdType.MESH
        )
        return carry

    lax.fori_loop(1, parts, greet, 0)

    low = lax.broadcasted_iota(jnp.int32, (1, LANES), 1) < head_size

    normed = layer_norm(tokens_ref[...].astype(jnp.float32), norm_gain_ref[...]).astype(jnp.bfloat16)
    front = jnp.dot(normed, w_proj_ref[:, width : 2 * width], preferred_element_type=jnp.float32)
    scaled = front.astype(jnp.bfloat16).astype(jnp.float32) * (0.5 * head_size ** (-0.5))
    back = jnp.dot(normed, w_proj_ref[:, 2 * width :], preferred_element_type=jnp.float32)
    for pair in range(heads // 2):
        cols = slice(pair * LANES, (pair + 1) * LANES)
        key_cols = back[:, :width][:, cols]
        value_cols = back[:, width:][:, cols]
        query_cols = scaled[:, cols]
        send_buf[2 * pair, :rows, :] = jnp.where(
            low, key_cols, pltpu.roll(value_cols, head_size, 1)
        ).astype(jnp.bfloat16)
        send_buf[2 * pair + 1, :rows, :] = jnp.where(
            low, pltpu.roll(key_cols, head_size, 1), value_cols
        ).astype(jnp.bfloat16)
        top, bottom = query_cols[:half], query_cols[half:]
        send_buf[2 * pair, rows:, :] = jnp.where(
            low, top, pltpu.roll(bottom, head_size, 1)
        ).astype(jnp.bfloat16)
        send_buf[2 * pair + 1, rows:, :] = jnp.where(
            low, pltpu.roll(top, head_size, 1), bottom
        ).astype(jnp.bfloat16)
    gate_proj = jnp.dot(normed, w_proj_ref[:, :width], preferred_element_type=jnp.float32)
    gate_buf[...] = jax.nn.silu(gate_proj).astype(jnp.bfloat16)

    pl.semaphore_wait(barrier, parts - 1)

    my_home = split_of(me)

    def payload(head, target):
        return pltpu.make_async_remote_copy(
            src_ref=send_buf.at[head],
            dst_ref=kvq.at[me],
            send_sem=send_sem.at[head],
            recv_sem=kv_sem.at[me],
            device_id={"pb": target},
            device_id_type=pl.DeviceIdType.MESH,
        )

    def each_payload(act):
        def one(step, carry):
            head = lax.rem(my_head + step, heads)
            target = head * splits + my_home

            @pl.when(target != me)
            def _():
                act(payload(head, target))

            return carry

        lax.fori_loop(0, heads, one, 0)

    def stamp_copy(target):
        return pltpu.make_async_remote_copy(
            src_ref=stamps_ref,
            dst_ref=stamp_all.at[me],
            send_sem=stamp_send_sem.at[target],
            recv_sem=stamp_sem.at[me],
            device_id={"pb": target},
            device_id_type=pl.DeviceIdType.MESH,
        )

    def stamp_arrival(source):
        return pltpu.make_async_remote_copy(
            src_ref=stamps_ref,
            dst_ref=stamp_all.at[source],
            send_sem=stamp_send_sem.at[source],
            recv_sem=stamp_sem.at[source],
            device_id={"pb": source},
            device_id_type=pl.DeviceIdType.MESH,
        )

    each_payload(lambda copy: copy.start())

    def send_stamps(step, carry):
        stamp_copy(lax.rem(me + step, parts)).start()
        return carry

    lax.fori_loop(1, parts, send_stamps, 0)

    stamp_all[me] = stamps_ref[...]

    @pl.when(my_home == my_split)
    def _():
        kvq[me] = send_buf[my_head]

    zeros_count = lax.broadcasted_iota(jnp.int32, (8, LANES), 1)
    bucket = jnp.clip((33 - zeros_count) >> 1, 0, buckets - 1)
    table = jnp.zeros((8, LANES), jnp.float32)
    for bucket_id in range(buckets):
        table = jnp.where(bucket == bucket_id, 0.5 * bias_ref[my_head, bucket_id], table)
    table = jnp.broadcast_to(table[:1], (rows, LANES))

    def arrival(source):
        return pltpu.make_async_remote_copy(
            src_ref=send_buf.at[0],
            dst_ref=kvq.at[source],
            send_sem=send_sem.at[0],
            recv_sem=kv_sem.at[source],
            device_id={"pb": source},
            device_id_type=pl.DeviceIdType.MESH,
        )

    def forward(slot, source, step):
        peer = my_head * splits + lax.rem(my_split + step, splits)
        return pltpu.make_async_remote_copy(
            src_ref=kvq.at[source, pl.ds(0, rows)],
            dst_ref=kvq.at[source, pl.ds(0, rows)],
            send_sem=fwd_sem.at[slot, step],
            recv_sem=kv_sem.at[source],
            device_id={"pb": peer},
            device_id_type=pl.DeviceIdType.MESH,
        )

    def take_direct(slot, carry):
        source = block_of(slot, my_split)

        @pl.when(source != me)
        def _():
            arrival(source).wait_recv()

        for step in range(1, splits):
            forward(slot, source, step).start()
        return carry

    lax.fori_loop(0, slots, take_direct, 0)

    def wait_stamps(step, carry):
        stamp_arrival(lax.rem(me + step, parts)).wait_recv()
        return carry

    lax.fori_loop(1, parts, wait_stamps, 0)

    for tile in range(parts // blocks_per_tile):
        stamp_keys[tile] = jnp.concatenate(
            [stamp_all[tile * blocks_per_tile + place] for place in range(blocks_per_tile)], axis=1
        )

    def send_back(slot, target):
        return pltpu.make_async_remote_copy(
            src_ref=back_buf.at[slot],
            dst_ref=att_buf.at[my_head],
            send_sem=back_sem.at[slot],
            recv_sem=att_sem.at[my_head],
            device_id={"pb": target},
            device_id_type=pl.DeviceIdType.MESH,
        )

    row_id = lax.broadcasted_iota(jnp.int32, (rows, LANES), 0)
    col_id = lax.broadcasted_iota(jnp.int32, (rows, LANES), 1)

    def one_slot(slot, carry):
        block = block_of(slot, my_split)
        for step in range(1, splits):
            source = block_of(slot, lax.rem(my_split + step, splits))
            forward(slot, source, step).wait_recv()
        packed = kvq[block, rows:, :].astype(jnp.float32)
        queries = jnp.concatenate(
            [jnp.where(low, packed, 0.0), jnp.where(low, pltpu.roll(packed, head_size, 1), 0.0)], axis=0
        ).astype(jnp.bfloat16)
        query_stamp = jnp.transpose(jnp.broadcast_to(stamp_all[block], (LANES, rows)))

        def visit(tile, total, masked):
            key_value = kvq[pl.ds(tile * blocks_per_tile, blocks_per_tile), :rows, :]
            key_value = key_value.reshape(key_tile, LANES)
            scores = lax.dot_general(
                queries, key_value, (((1,), (1,)), ((), ())), preferred_element_type=jnp.float32
            )
            weights = []
            for first in range(0, key_tile, LANES):
                elapsed = query_stamp - stamp_keys[tile, :, first : first + LANES]
                bias = jnp.take_along_axis(table, lax.clz(elapsed), axis=1, mode="promise_in_bounds")
                halved = scores[:, first : first + LANES] + bias
                weight = halved + halved * jnp.tanh(halved)
                if masked:
                    ahead = tile * key_tile + first - block * rows
                    weight = jnp.where(col_id + ahead <= row_id, weight, 0.0)
                weights.append(weight.astype(jnp.bfloat16))
            return total + jnp.dot(
                jnp.concatenate(weights, axis=1), key_value, preferred_element_type=jnp.float32
            )

        last = block // blocks_per_tile
        total = lax.fori_loop(
            0, last, lambda tile, total: visit(tile, total, False), jnp.zeros((rows, LANES), jnp.float32)
        )
        total = visit(last, total, True)
        result = jnp.where(low, pltpu.roll(total[:half], head_size, 1), total[half:]).astype(jnp.bfloat16)
        back_buf[slot] = result

        @pl.when(block == me)
        def _():
            att_buf[my_head] = result

        @pl.when(block != me)
        def _():
            send_back(slot, block).start()

        return carry

    lax.fori_loop(0, slots, one_slot, 0)

    each_payload(lambda copy: copy.wait_send())

    def drain(step, carry):
        stamp_copy(lax.rem(me + step, parts)).wait_send()
        return carry

    lax.fori_loop(1, parts, drain, 0)

    def drain_slot(slot, carry):
        source = block_of(slot, my_split)
        for step in range(1, splits):
            forward(slot, source, step).wait_send()

        @pl.when(source != me)
        def _():
            send_back(slot, source).wait_send()

        return carry

    lax.fori_loop(0, slots, drain_slot, 0)

    def take_back(step, carry):
        head = lax.rem(my_head + step, heads)
        source = head * splits + my_home

        @pl.when(source != me)
        def _():
            pltpu.make_async_remote_copy(
                src_ref=back_buf.at[0],
                dst_ref=att_buf.at[head],
                send_sem=back_sem.at[0],
                recv_sem=att_sem.at[head],
                device_id={"pb": source},
                device_id_type=pl.DeviceIdType.MESH,
            ).wait_recv()

        return carry

    lax.fori_loop(0, heads, take_back, 0)

    pieces = []
    for pair in range(heads // 2):
        even = att_buf[2 * pair].astype(jnp.float32)
        odd = att_buf[2 * pair + 1].astype(jnp.float32)
        pieces.append(
            jnp.concatenate(
                [
                    jnp.where(low, even, pltpu.roll(odd, head_size, 1)),
                    jnp.where(low, pltpu.roll(even, head_size, 1), odd),
                ],
                axis=0,
            )
        )
    attended = jnp.concatenate(pieces, axis=1)
    gated = layer_norm(attended, attn_gain_ref[...]) * gate_buf[...].astype(jnp.float32)
    mixed = tokens_ref[...].astype(jnp.float32) + jnp.dot(
        gated.astype(jnp.bfloat16), w_out_ref[...], preferred_element_type=jnp.float32
    )
    out_ref[...] = mixed.astype(jnp.bfloat16)


def solution(mesh):
    parts = mesh.shape["pb"]

    def body(tokens, stamps, norm_gain, w_proj, rel_bias, attn_gain, w_out):
        rows, width = tokens.shape
        heads = rel_bias.shape[0]
        splits = parts // heads
        slots = parts // splits
        blocks_per_tile = max(1, 384 // rows)
        vmem = pl.BlockSpec(memory_space=pltpu.VMEM)
        smem = pl.BlockSpec(memory_space=pltpu.SMEM)
        return pl.pallas_call(
            functools.partial(kernel, parts, heads),
            out_shape=jax.ShapeDtypeStruct((rows, width), jnp.bfloat16),
            in_specs=[vmem, vmem, vmem, vmem, smem, vmem, vmem],
            out_specs=vmem,
            scratch_shapes=[
                pltpu.VMEM((heads, rows + rows // 2, LANES), jnp.bfloat16),
                pltpu.VMEM((parts, rows + rows // 2, LANES), jnp.bfloat16),
                pltpu.VMEM((parts, 1, rows), jnp.int32),
                pltpu.VMEM((parts // blocks_per_tile, 1, blocks_per_tile * rows), jnp.int32),
                pltpu.VMEM((rows, width), jnp.bfloat16),
                pltpu.VMEM((slots, rows // 2, LANES), jnp.bfloat16),
                pltpu.VMEM((heads, rows // 2, LANES), jnp.bfloat16),
                pltpu.SemaphoreType.DMA((heads,)),
                pltpu.SemaphoreType.DMA((slots, splits)),
                pltpu.SemaphoreType.DMA((parts,)),
                pltpu.SemaphoreType.DMA((parts,)),
                pltpu.SemaphoreType.DMA((parts,)),
                pltpu.SemaphoreType.DMA((slots,)),
                pltpu.SemaphoreType.DMA((heads,)),
            ],
            compiler_params=pltpu.CompilerParams(
                collective_id=0, has_side_effects=True, vmem_limit_bytes=48 * 1024 * 1024
            ),
        )(
            tokens,
            stamps.reshape(1, rows),
            norm_gain.reshape(1, width),
            w_proj,
            rel_bias,
            attn_gain.reshape(1, width),
            w_out,
        )

    return jax.shard_map(
        body,
        mesh=mesh,
        in_specs=(P(("groups", "pb"), None), P(("groups", "pb")), P(), P(), P(), P(), P()),
        out_specs=P(("groups", "pb"), None),
        check_vma=False,
    )
```

```python
import functools

import jax
import jax.numpy as jnp
from jax import lax
from jax.experimental import pallas as pl
from jax.experimental.pallas import tpu as pltpu
from jax.sharding import PartitionSpec as P

EPSILON = 1e-05
LANES = 128


def layer_norm(values, gain):
    centered = values - jnp.mean(values, axis=-1, keepdims=True)
    spread = jnp.mean(centered * centered, axis=-1, keepdims=True)
    return centered * lax.rsqrt(spread + EPSILON) * gain


def kernel(
    parts,
    heads,
    tokens_hbm,
    stamps_hbm,
    norm_gain_hbm,
    w_proj_hbm,
    bias_hbm,
    attn_gain_hbm,
    w_out_hbm,
    out_ref,
    tokens_ref,
    stamps_ref,
    norm_gain_ref,
    w_proj_ref,
    bias_ref,
    attn_gain_ref,
    w_out_ref,
    kv_send,
    q_send,
    kv_all,
    q_all,
    query_buf,
    stamp_all,
    stamp_keys,
    stamp_rows,
    total_buf,
    gate_buf,
    back_buf,
    att_buf,
    load_sem,
    kv_send_sem,
    q_send_sem,
    fwd_sem,
    kv_sem,
    q_sem,
    stamp_send_sem,
    stamp_sem,
    back_sem,
    att_sem,
):
    rows, width = tokens_ref.shape
    half = rows // 2
    head_size = width // heads
    splits = parts // heads
    slots = heads
    near = slots // 2
    blocks_per_tile = max(1, 384 // rows)
    key_tile = blocks_per_tile * rows
    group_tiles = splits // blocks_per_tile
    buckets = bias_ref.shape[1]

    loads = [
        pltpu.make_async_copy(source, target, load_sem.at[index])
        for index, (source, target) in enumerate(
            [
                (tokens_hbm, tokens_ref),
                (norm_gain_hbm, norm_gain_ref),
                (w_proj_hbm.at[:, width:], w_proj_ref.at[:, width:]),
                (stamps_hbm, stamps_ref),
                (bias_hbm, bias_ref),
                (w_proj_hbm.at[:, :width], w_proj_ref.at[:, :width]),
                (attn_gain_hbm, attn_gain_ref),
                (w_out_hbm, w_out_ref),
            ]
        )
    ]
    for load in loads:
        load.start()

    me = lax.axis_index("pb")
    my_head = me // splits
    my_split = me % splits
    upper = my_head // near
    my_place = my_head % near
    near_first = upper * near
    far_first = near - near_first

    def split_of(block):
        place = block % splits
        odd = (block // splits) % 2
        return place + odd * (splits - 1 - 2 * place)

    def block_of(slot, split):
        odd = slot % 2
        return slot * splits + split + odd * (splits - 1 - 2 * split)

    def remote(source, target, send, receive, device):
        return pltpu.make_async_remote_copy(
            src_ref=source,
            dst_ref=target,
            send_sem=send,
            recv_sem=receive,
            device_id={"pb": device},
            device_id_type=pl.DeviceIdType.MESH,
        )

    barrier = pltpu.get_barrier_semaphore()

    def greet(step, carry):
        other = lax.rem(me + step, parts)
        pl.semaphore_signal(
            barrier, inc=1, device_id={"pb": other}, device_id_type=pl.DeviceIdType.MESH
        )
        return carry

    lax.fori_loop(1, parts, greet, 0)

    low = lax.broadcasted_iota(jnp.int32, (1, LANES), 1) < head_size

    for load in loads[:3]:
        load.wait()
    normed = layer_norm(tokens_ref[...].astype(jnp.float32), norm_gain_ref[...]).astype(jnp.bfloat16)
    front = jnp.dot(normed, w_proj_ref[:, width : 2 * width], preferred_element_type=jnp.float32)
    scaled = front.astype(jnp.bfloat16).astype(jnp.float32) * (0.5 * head_size ** (-0.5))
    back = jnp.dot(normed, w_proj_ref[:, 2 * width :], preferred_element_type=jnp.float32)
    for pair in range(heads // 2):
        cols = slice(pair * LANES, (pair + 1) * LANES)
        key_cols = back[:, :width][:, cols]
        value_cols = back[:, width:][:, cols]
        query_cols = scaled[:, cols]
        kv_send[2 * pair] = jnp.where(
            low, key_cols, pltpu.roll(value_cols, head_size, 1)
        ).astype(jnp.bfloat16)
        kv_send[2 * pair + 1] = jnp.where(
            low, pltpu.roll(key_cols, head_size, 1), value_cols
        ).astype(jnp.bfloat16)
        top, bottom = query_cols[:half], query_cols[half:]
        q_send[2 * pair] = jnp.where(low, top, pltpu.roll(bottom, head_size, 1)).astype(jnp.bfloat16)
        q_send[2 * pair + 1] = jnp.where(low, pltpu.roll(top, head_size, 1), bottom).astype(jnp.bfloat16)
    loads[3].wait()
    loads[4].wait()

    my_home = split_of(me)

    def stamp_copy(target):
        return remote(
            stamps_ref, stamp_all.at[me], stamp_send_sem.at[target], stamp_sem.at[me], target
        )

    def kv_copy(head, target):
        return remote(kv_send.at[head], kv_all.at[me], kv_send_sem.at[head], kv_sem.at[me], target)

    def q_copy(head, target):
        return remote(q_send.at[head], q_all.at[my_head], q_send_sem.at[head], q_sem.at[my_head], target)

    def each_head(first, act):
        def one(step, carry):
            head = first + lax.rem(my_place + step, near)
            target = head * splits + my_home

            @pl.when(target != me)
            def _():
                act(head, target)

            return carry

        lax.fori_loop(0, near, one, 0)

    def send_stamps(step, carry):
        stamp_copy(lax.rem(me + step, parts)).start()
        return carry

    def start_both(head, target):
        q_copy(head, target).start()
        kv_copy(head, target).start()

    pl.semaphore_wait(barrier, parts - 1)
    lax.fori_loop(1, parts, send_stamps, 0)
    each_head(near_first, start_both)
    each_head(far_first, lambda head, target: q_copy(head, target).start())
    each_head(far_first, lambda head, target: kv_copy(head, target).start())

    stamp_all[me] = stamps_ref[...]

    @pl.when(my_home == my_split)
    def _():
        kv_all[me] = kv_send[my_head]
        q_all[my_head] = q_send[my_head]

    loads[5].wait()
    gate_proj = jnp.dot(normed, w_proj_ref[:, :width], preferred_element_type=jnp.float32)
    gate_buf[...] = jax.nn.silu(gate_proj).astype(jnp.bfloat16)
    total_buf[...] = jnp.zeros_like(total_buf)

    zeros_count = lax.broadcasted_iota(jnp.int32, (8, LANES), 1)
    bucket = jnp.clip((33 - zeros_count) >> 1, 0, buckets - 1)
    table = jnp.zeros((8, LANES), jnp.float32)
    for bucket_id in range(buckets):
        table = jnp.where(bucket == bucket_id, 0.5 * bias_ref[my_head, bucket_id], table)
    table = jnp.broadcast_to(table[:1], (rows, LANES))

    def wait_stamps(step, carry):
        source = lax.rem(me + step, parts)
        remote(
            stamps_ref, stamp_all.at[source], stamp_send_sem.at[source], stamp_sem.at[source], source
        ).wait_recv()
        return carry

    lax.fori_loop(1, parts, wait_stamps, 0)

    for tile in range(parts // blocks_per_tile):
        stamp_keys[tile] = jnp.concatenate(
            [stamp_all[tile * blocks_per_tile + place] for place in range(blocks_per_tile)], axis=1
        )

    def turn_stamps(slot, carry):
        block = block_of(slot, my_split)
        stamp_rows[slot] = jnp.transpose(jnp.broadcast_to(stamp_all[block], (LANES, rows)))
        return carry

    lax.fori_loop(0, slots, turn_stamps, 0)

    def forward(slot, source, step):
        peer = my_head * splits + lax.rem(my_split + step, splits)
        return remote(
            kv_all.at[source], kv_all.at[source], fwd_sem.at[slot, step], kv_sem.at[source], peer
        )

    def take_direct(slot):
        source = block_of(slot, my_split)

        @pl.when(source != me)
        def _():
            remote(
                kv_send.at[0], kv_all.at[source], kv_send_sem.at[0], kv_sem.at[source], source
            ).wait_recv()

        for step in range(1, splits):
            forward(slot, source, step).start()

    def take_forwarded(slot):
        for step in range(1, splits):
            source = block_of(slot, lax.rem(my_split + step, splits))
            forward(slot, source, step).wait_recv()

    def take_query(slot):
        source = block_of(slot, my_split)

        @pl.when(source != me)
        def _():
            remote(
                q_send.at[0], q_all.at[slot], q_send_sem.at[0], q_sem.at[slot], source
            ).wait_recv()

        packed = q_all[slot].astype(jnp.float32)
        query_buf[slot] = jnp.concatenate(
            [jnp.where(low, packed, 0.0), jnp.where(low, pltpu.roll(packed, head_size, 1), 0.0)], axis=0
        ).astype(jnp.bfloat16)

    row_id = lax.broadcasted_iota(jnp.int32, (rows, LANES), 0)
    col_id = lax.broadcasted_iota(jnp.int32, (rows, LANES), 1)

    def visit_tile(slot, block, tile, masked):
        key_value = kv_all[pl.ds(tile * blocks_per_tile, blocks_per_tile)]
        key_value = key_value.reshape(key_tile, LANES)
        scores = lax.dot_general(
            query_buf[slot], key_value, (((1,), (1,)), ((), ())), preferred_element_type=jnp.float32
        )
        query_stamp = stamp_rows[slot]
        weights = []
        for first in range(0, key_tile, LANES):
            elapsed = query_stamp - stamp_keys[tile, :, first : first + LANES]
            bias = jnp.take_along_axis(table, lax.clz(elapsed), axis=1, mode="promise_in_bounds")
            halved = scores[:, first : first + LANES] + bias
            weight = halved + halved * jnp.tanh(halved)
            if masked:
                ahead = tile * key_tile + first - block * rows
                weight = jnp.where(col_id + ahead <= row_id, weight, 0.0)
            weights.append(weight.astype(jnp.bfloat16))
        total_buf[slot] += jnp.dot(
            jnp.concatenate(weights, axis=1), key_value, preferred_element_type=jnp.float32
        )

    def visit_before(slot, group):
        def one(tile, carry):
            visit_tile(slot, 0, tile, False)
            return carry

        lax.fori_loop(group * group_tiles, (group + 1) * group_tiles, one, 0)

    def visit_own(slot):
        block = block_of(slot, my_split)
        last = block // blocks_per_tile

        def one(tile, carry):
            visit_tile(slot, block, tile, False)
            return carry

        if group_tiles > 1:
            lax.fori_loop(slot * group_tiles, last, one, 0)
        visit_tile(slot, block, last, True)

    def send_back(slot, target):
        return remote(
            back_buf.at[slot], att_buf.at[my_head], back_sem.at[slot], att_sem.at[my_head], target
        )

    def finish(slot, carry):
        block = block_of(slot, my_split)
        total = total_buf[slot]
        result = jnp.where(low, pltpu.roll(total[:half], head_size, 1), total[half:]).astype(jnp.bfloat16)
        back_buf[slot] = result

        @pl.when(block == me)
        def _():
            att_buf[my_head] = result

        @pl.when(block != me)
        def _():
            send_back(slot, block).start()

        return carry

    def take_near(slot, carry):
        take_direct(slot)
        take_query(slot)
        return carry

    lax.fori_loop(near_first, near_first + near, take_near, 0)

    def near_group(group, carry):
        take_forwarded(group)
        visit_own(group)

        def one(slot, inner):
            visit_before(slot, group)
            return inner

        lax.fori_loop(group + 1, near_first + near, one, 0)
        return carry

    lax.fori_loop(near_first, near_first + near, near_group, 0)

    lower_end = near * (1 - upper)
    lax.fori_loop(0, lower_end, finish, 0)

    def far_query(slot, carry):
        take_query(slot)
        return carry

    def later_query(step, carry):
        slot = near + step
        take_query(slot)

        def one(group, inner):
            visit_before(slot, group)
            return inner

        lax.fori_loop(0, near, one, 0)
        return carry

    lax.fori_loop(0, lower_end, later_query, 0)
    lax.fori_loop(0, near * upper, far_query, 0)

    def far_at(step):
        return far_first + lax.rem(my_place - step + near, near)

    take_direct(far_at(0))

    def far_group(step, carry):
        group = far_at(step)
        take_forwarded(group)
        visit_own(group)

        def one(slot, inner):
            visit_before(slot, group)
            return inner

        lax.fori_loop(group + 1, slots, one, 0)

        @pl.when(step + 1 < near)
        def _():
            take_direct(far_at(step + 1))

        return carry

    lax.fori_loop(0, near, far_group, 0)
    lax.fori_loop(lower_end, slots, finish, 0)

    def drain_both(head, target):
        q_copy(head, target).wait_send()
        kv_copy(head, target).wait_send()

    each_head(near_first, drain_both)
    each_head(far_first, drain_both)

    def drain(step, carry):
        stamp_copy(lax.rem(me + step, parts)).wait_send()
        return carry

    lax.fori_loop(1, parts, drain, 0)

    def drain_slot(slot, carry):
        source = block_of(slot, my_split)
        for step in range(1, splits):
            forward(slot, source, step).wait_send()

        @pl.when(source != me)
        def _():
            send_back(slot, source).wait_send()

        return carry

    lax.fori_loop(0, slots, drain_slot, 0)
    loads[6].wait()
    loads[7].wait()

    def take_back(step, carry):
        head = lax.rem(my_head + step, heads)
        source = head * splits + my_home

        @pl.when(source != me)
        def _():
            remote(
                back_buf.at[0], att_buf.at[head], back_sem.at[0], att_sem.at[head], source
            ).wait_recv()

        return carry

    lax.fori_loop(0, heads, take_back, 0)

    pieces = []
    for pair in range(heads // 2):
        even = att_buf[2 * pair].astype(jnp.float32)
        odd = att_buf[2 * pair + 1].astype(jnp.float32)
        pieces.append(
            jnp.concatenate(
                [
                    jnp.where(low, even, pltpu.roll(odd, head_size, 1)),
                    jnp.where(low, pltpu.roll(even, head_size, 1), odd),
                ],
                axis=0,
            )
        )
    attended = jnp.concatenate(pieces, axis=1)
    gated = layer_norm(attended, attn_gain_ref[...]) * gate_buf[...].astype(jnp.float32)
    mixed = tokens_ref[...].astype(jnp.float32) + jnp.dot(
        gated.astype(jnp.bfloat16), w_out_ref[...], preferred_element_type=jnp.float32
    )
    out_ref[...] = mixed.astype(jnp.bfloat16)


def solution(mesh):
    parts = mesh.shape["pb"]

    def body(tokens, stamps, norm_gain, w_proj, rel_bias, attn_gain, w_out):
        rows, width = tokens.shape
        heads = rel_bias.shape[0]
        splits = parts // heads
        slots = parts // splits
        blocks_per_tile = max(1, 384 // rows)
        vmem = pl.BlockSpec(memory_space=pltpu.VMEM)
        return pl.pallas_call(
            functools.partial(kernel, parts, heads),
            out_shape=jax.ShapeDtypeStruct((rows, width), jnp.bfloat16),
            in_specs=[pl.BlockSpec(memory_space=pltpu.HBM)] * 7,
            out_specs=vmem,
            scratch_shapes=[
                pltpu.VMEM((rows, width), jnp.bfloat16),
                pltpu.VMEM((1, rows), jnp.int32),
                pltpu.VMEM((1, width), jnp.float32),
                pltpu.VMEM(w_proj.shape, jnp.bfloat16),
                pltpu.SMEM(rel_bias.shape, jnp.float32),
                pltpu.VMEM((1, width), jnp.float32),
                pltpu.VMEM(w_out.shape, jnp.bfloat16),
                pltpu.VMEM((heads, rows, LANES), jnp.bfloat16),
                pltpu.VMEM((heads, rows // 2, LANES), jnp.bfloat16),
                pltpu.VMEM((parts, rows, LANES), jnp.bfloat16),
                pltpu.VMEM((slots, rows // 2, LANES), jnp.bfloat16),
                pltpu.VMEM((slots, rows, LANES), jnp.bfloat16),
                pltpu.VMEM((parts, 1, rows), jnp.int32),
                pltpu.VMEM((parts // blocks_per_tile, 1, blocks_per_tile * rows), jnp.int32),
                pltpu.VMEM((slots, rows, LANES), jnp.int32),
                pltpu.VMEM((slots, rows, LANES), jnp.float32),
                pltpu.VMEM((rows, width), jnp.bfloat16),
                pltpu.VMEM((slots, rows // 2, LANES), jnp.bfloat16),
                pltpu.VMEM((heads, rows // 2, LANES), jnp.bfloat16),
                pltpu.SemaphoreType.DMA((8,)),
                pltpu.SemaphoreType.DMA((heads,)),
                pltpu.SemaphoreType.DMA((heads,)),
                pltpu.SemaphoreType.DMA((slots, splits)),
                pltpu.SemaphoreType.DMA((parts,)),
                pltpu.SemaphoreType.DMA((slots,)),
                pltpu.SemaphoreType.DMA((parts,)),
                pltpu.SemaphoreType.DMA((parts,)),
                pltpu.SemaphoreType.DMA((slots,)),
                pltpu.SemaphoreType.DMA((heads,)),
            ],
            compiler_params=pltpu.CompilerParams(
                collective_id=0, has_side_effects=True
            ),
        )(
            tokens,
            stamps.reshape(1, rows),
            norm_gain.reshape(1, width),
            w_proj,
            rel_bias,
            attn_gain.reshape(1, width),
            w_out,
        )

    return jax.shard_map(
        body,
        mesh=mesh,
        in_specs=(P(("groups", "pb"), None), P(("groups", "pb")), P(), P(), P(), P(), P()),
        out_specs=P(("groups", "pb"), None),
        check_vma=False,
    )
```

```python
import functools

import jax
import jax.numpy as jnp
from jax import lax
from jax.experimental import pallas as pl
from jax.experimental.pallas import tpu as pltpu
from jax.sharding import PartitionSpec as P

EPSILON = 1e-05
LANES = 128


def layer_norm(values, gain):
    centered = values - jnp.mean(values, axis=-1, keepdims=True)
    spread = jnp.mean(centered * centered, axis=-1, keepdims=True)
    return centered * lax.rsqrt(spread + EPSILON) * gain


def kernel(
    parts,
    heads,
    tokens_hbm,
    stamps_hbm,
    norm_gain_hbm,
    w_proj_hbm,
    bias_hbm,
    attn_gain_hbm,
    w_out_hbm,
    out_ref,
    tokens_ref,
    stamps_ref,
    norm_gain_ref,
    w_proj_ref,
    bias_ref,
    attn_gain_ref,
    w_out_ref,
    kv_send,
    q_send,
    kv_all,
    q_all,
    query_buf,
    stamp_all,
    stamp_keys,
    stamp_rows,
    total_buf,
    gate_buf,
    back_buf,
    att_buf,
    load_sem,
    kv_send_sem,
    q_send_sem,
    fwd_sem,
    kv_sem,
    q_sem,
    stamp_send_sem,
    stamp_sem,
    back_sem,
    att_sem,
):
    rows, width = tokens_ref.shape
    half = rows // 2
    head_size = width // heads
    splits = parts // heads
    slots = heads
    near = slots // 2
    blocks_per_tile = max(1, 384 // rows)
    key_tile = blocks_per_tile * rows
    group_tiles = splits // blocks_per_tile
    buckets = bias_ref.shape[1]

    loads = [
        pltpu.make_async_copy(source, target, load_sem.at[index])
        for index, (source, target) in enumerate(
            [
                (tokens_hbm, tokens_ref),
                (norm_gain_hbm, norm_gain_ref),
                (w_proj_hbm.at[:, width:], w_proj_ref.at[:, width:]),
                (stamps_hbm, stamps_ref),
                (bias_hbm, bias_ref),
                (w_proj_hbm.at[:, :width], w_proj_ref.at[:, :width]),
                (attn_gain_hbm, attn_gain_ref),
                (w_out_hbm, w_out_ref),
            ]
        )
    ]
    for load in loads:
        load.start()

    me = lax.axis_index("pb")
    my_head = me // splits
    my_split = me % splits
    upper = my_head // near
    my_place = my_head % near
    near_first = upper * near
    far_first = near - near_first

    def split_of(block):
        place = block % splits
        odd = (block // splits) % 2
        return place + odd * (splits - 1 - 2 * place)

    def block_of(slot, split):
        odd = slot % 2
        return slot * splits + split + odd * (splits - 1 - 2 * split)

    def remote(source, target, send, receive, device):
        return pltpu.make_async_remote_copy(
            src_ref=source,
            dst_ref=target,
            send_sem=send,
            recv_sem=receive,
            device_id={"pb": device},
            device_id_type=pl.DeviceIdType.MESH,
        )

    barrier = pltpu.get_barrier_semaphore()

    def greet(step, carry):
        other = lax.rem(me + step, parts)
        pl.semaphore_signal(
            barrier, inc=1, device_id={"pb": other}, device_id_type=pl.DeviceIdType.MESH
        )
        return carry

    lax.fori_loop(1, parts, greet, 0)

    low = lax.broadcasted_iota(jnp.int32, (1, LANES), 1) < head_size

    for load in loads[:3]:
        load.wait()
    normed = layer_norm(tokens_ref[...].astype(jnp.float32), norm_gain_ref[...]).astype(jnp.bfloat16)
    front = jnp.dot(normed, w_proj_ref[:, width : 2 * width], preferred_element_type=jnp.float32)
    scaled = front.astype(jnp.bfloat16).astype(jnp.float32) * (0.5 * head_size ** (-0.5))
    back = jnp.dot(normed, w_proj_ref[:, 2 * width :], preferred_element_type=jnp.float32)
    for pair in range(heads // 2):
        cols = slice(pair * LANES, (pair + 1) * LANES)
        key_cols = back[:, :width][:, cols]
        value_cols = back[:, width:][:, cols]
        query_cols = scaled[:, cols]
        kv_send[2 * pair] = jnp.where(
            low, key_cols, pltpu.roll(value_cols, head_size, 1)
        ).astype(jnp.bfloat16)
        kv_send[2 * pair + 1] = jnp.where(
            low, pltpu.roll(key_cols, head_size, 1), value_cols
        ).astype(jnp.bfloat16)
        top, bottom = query_cols[:half], query_cols[half:]
        q_send[2 * pair] = jnp.where(low, top, pltpu.roll(bottom, head_size, 1)).astype(jnp.bfloat16)
        q_send[2 * pair + 1] = jnp.where(low, pltpu.roll(top, head_size, 1), bottom).astype(jnp.bfloat16)
    loads[3].wait()
    loads[4].wait()

    my_home = split_of(me)

    def stamp_copy(target):
        return remote(
            stamps_ref, stamp_all.at[me], stamp_send_sem.at[target], stamp_sem.at[me], target
        )

    def kv_copy(head, target):
        return remote(kv_send.at[head], kv_all.at[me], kv_send_sem.at[head], kv_sem.at[me], target)

    def q_copy(head, target):
        return remote(q_send.at[head], q_all.at[my_head], q_send_sem.at[head], q_sem.at[my_head], target)

    def each_head(first, act):
        def one(step, carry):
            head = first + lax.rem(my_place + step, near)
            target = head * splits + my_home

            @pl.when(target != me)
            def _():
                act(head, target)

            return carry

        lax.fori_loop(0, near, one, 0)

    def send_stamps(step, carry):
        stamp_copy(lax.rem(me + step, parts)).start()
        return carry

    def start_both(head, target):
        q_copy(head, target).start()
        kv_copy(head, target).start()

    pl.semaphore_wait(barrier, parts - 1)
    lax.fori_loop(1, parts, send_stamps, 0)
    each_head(near_first, start_both)
    each_head(far_first, lambda head, target: q_copy(head, target).start())
    each_head(far_first, lambda head, target: kv_copy(head, target).start())

    stamp_all[me] = stamps_ref[...]

    @pl.when(my_home == my_split)
    def _():
        kv_all[me] = kv_send[my_head]
        q_all[my_head] = q_send[my_head]

    loads[5].wait()
    gate_proj = jnp.dot(normed, w_proj_ref[:, :width], preferred_element_type=jnp.float32)
    gate_buf[...] = jax.nn.silu(gate_proj).astype(jnp.bfloat16)
    total_buf[...] = jnp.zeros_like(total_buf)

    zeros_count = lax.broadcasted_iota(jnp.int32, (8, LANES), 1)
    bucket = jnp.clip((33 - zeros_count) >> 1, 0, buckets - 1)
    table = jnp.zeros((8, LANES), jnp.float32)
    for bucket_id in range(buckets):
        table = jnp.where(bucket == bucket_id, 0.5 * bias_ref[my_head, bucket_id], table)
    table = jnp.broadcast_to(table[:1], (rows, LANES))

    def wait_stamps(step, carry):
        source = lax.rem(me + step, parts)
        remote(
            stamps_ref, stamp_all.at[source], stamp_send_sem.at[source], stamp_sem.at[source], source
        ).wait_recv()
        return carry

    lax.fori_loop(1, parts, wait_stamps, 0)

    for tile in range(parts // blocks_per_tile):
        stamp_keys[tile] = jnp.concatenate(
            [stamp_all[tile * blocks_per_tile + place] for place in range(blocks_per_tile)], axis=1
        )

    def turn_stamps(slot, carry):
        block = block_of(slot, my_split)
        stamp_rows[slot] = jnp.transpose(jnp.broadcast_to(stamp_all[block], (LANES, rows)))
        return carry

    lax.fori_loop(0, slots, turn_stamps, 0)

    def forward(slot, source, step):
        peer = my_head * splits + lax.rem(my_split + step, splits)
        return remote(
            kv_all.at[source], kv_all.at[source], fwd_sem.at[slot, step], kv_sem.at[source], peer
        )

    def take_direct(slot):
        source = block_of(slot, my_split)

        @pl.when(source != me)
        def _():
            remote(
                kv_send.at[0], kv_all.at[source], kv_send_sem.at[0], kv_sem.at[source], source
            ).wait_recv()

        for step in range(1, splits):
            forward(slot, source, step).start()

    def take_forwarded(slot):
        for step in range(1, splits):
            source = block_of(slot, lax.rem(my_split + step, splits))
            forward(slot, source, step).wait_recv()

    def take_query(slot):
        source = block_of(slot, my_split)

        @pl.when(source != me)
        def _():
            remote(
                q_send.at[0], q_all.at[slot], q_send_sem.at[0], q_sem.at[slot], source
            ).wait_recv()

        packed = q_all[slot].astype(jnp.float32)
        query_buf[slot] = jnp.concatenate(
            [jnp.where(low, packed, 0.0), jnp.where(low, pltpu.roll(packed, head_size, 1), 0.0)], axis=0
        ).astype(jnp.bfloat16)

    row_id = lax.broadcasted_iota(jnp.int32, (rows, LANES), 0)
    col_id = lax.broadcasted_iota(jnp.int32, (rows, LANES), 1)

    def visit_tile(slot, block, tile, masked):
        key_value = kv_all[pl.ds(tile * blocks_per_tile, blocks_per_tile)]
        key_value = key_value.reshape(key_tile, LANES)
        scores = lax.dot_general(
            query_buf[slot], key_value, (((1,), (1,)), ((), ())), preferred_element_type=jnp.float32
        )
        query_stamp = stamp_rows[slot]
        weights = []
        for first in range(0, key_tile, LANES):
            elapsed = query_stamp - stamp_keys[tile, :, first : first + LANES]
            bias = jnp.take_along_axis(table, lax.clz(elapsed), axis=1, mode="promise_in_bounds")
            halved = scores[:, first : first + LANES] + bias
            weight = halved + halved * jnp.tanh(halved)
            if masked:
                ahead = tile * key_tile + first - block * rows
                weight = jnp.where(col_id + ahead <= row_id, weight, 0.0)
            weights.append(weight.astype(jnp.bfloat16))
        total_buf[slot] += jnp.dot(
            jnp.concatenate(weights, axis=1), key_value, preferred_element_type=jnp.float32
        )

    def visit_before(slot, group):
        def one(tile, carry):
            visit_tile(slot, 0, tile, False)
            return carry

        lax.fori_loop(group * group_tiles, (group + 1) * group_tiles, one, 0)

    def visit_own(slot):
        block = block_of(slot, my_split)
        last = block // blocks_per_tile

        def one(tile, carry):
            visit_tile(slot, block, tile, False)
            return carry

        if group_tiles > 1:
            lax.fori_loop(slot * group_tiles, last, one, 0)
        visit_tile(slot, block, last, True)

    def send_back(slot, target):
        return remote(
            back_buf.at[slot], att_buf.at[my_head], back_sem.at[slot], att_sem.at[my_head], target
        )

    def finish(slot, carry):
        block = block_of(slot, my_split)
        total = total_buf[slot]
        result = jnp.where(low, pltpu.roll(total[:half], head_size, 1), total[half:]).astype(jnp.bfloat16)
        back_buf[slot] = result

        @pl.when(block == me)
        def _():
            att_buf[my_head] = result

        @pl.when(block != me)
        def _():
            send_back(slot, block).start()

        return carry

    def take_near(slot, carry):
        take_direct(slot)
        take_query(slot)
        return carry

    lax.fori_loop(near_first, near_first + near, take_near, 0)

    def near_group(group, carry):
        take_forwarded(group)
        visit_own(group)

        def one(slot, inner):
            visit_before(slot, group)
            return inner

        lax.fori_loop(group + 1, near_first + near, one, 0)
        return carry

    lax.fori_loop(near_first, near_first + near, near_group, 0)

    lower_end = near * (1 - upper)
    lax.fori_loop(0, lower_end, finish, 0)

    def far_query(slot, carry):
        take_query(slot)
        return carry

    def later_query(step, carry):
        slot = near + step
        take_query(slot)

        def one(group, inner):
            visit_before(slot, group)
            return inner

        lax.fori_loop(0, near, one, 0)
        return carry

    lax.fori_loop(0, lower_end, later_query, 0)
    lax.fori_loop(0, near * upper, far_query, 0)

    def far_at(step):
        return far_first + lax.rem(my_place - step + near, near)

    take_direct(far_at(0))

    def far_group(step, carry):
        group = far_at(step)
        take_forwarded(group)

        def one(slot, inner):
            visit_before(slot, group)
            return inner

        @pl.when(step + 1 < near)
        def _():
            take_direct(far_at(step + 1))

        visit_own(group)
        lax.fori_loop(group + 1, slots, one, 0)
        return carry

    lax.fori_loop(0, near - 1, far_group, 0)

    last_group = far_at(near - 1)
    lax.fori_loop(lower_end, last_group, finish, 0)
    take_forwarded(last_group)
    visit_own(last_group)
    finish(last_group, 0)

    def last_one(slot, carry):
        visit_before(slot, last_group)
        return finish(slot, carry)

    lax.fori_loop(last_group + 1, slots, last_one, 0)

    def drain_both(head, target):
        q_copy(head, target).wait_send()
        kv_copy(head, target).wait_send()

    each_head(near_first, drain_both)
    each_head(far_first, drain_both)

    def drain(step, carry):
        stamp_copy(lax.rem(me + step, parts)).wait_send()
        return carry

    lax.fori_loop(1, parts, drain, 0)

    def drain_slot(slot, carry):
        source = block_of(slot, my_split)
        for step in range(1, splits):
            forward(slot, source, step).wait_send()

        @pl.when(source != me)
        def _():
            send_back(slot, source).wait_send()

        return carry

    lax.fori_loop(0, slots, drain_slot, 0)
    loads[6].wait()
    loads[7].wait()

    def take_back(step, carry):
        head = lax.rem(my_head + step, heads)
        source = head * splits + my_home

        @pl.when(source != me)
        def _():
            remote(
                back_buf.at[0], att_buf.at[head], back_sem.at[0], att_sem.at[head], source
            ).wait_recv()

        return carry

    lax.fori_loop(0, heads, take_back, 0)

    pieces = []
    for pair in range(heads // 2):
        even = att_buf[2 * pair].astype(jnp.float32)
        odd = att_buf[2 * pair + 1].astype(jnp.float32)
        pieces.append(
            jnp.concatenate(
                [
                    jnp.where(low, even, pltpu.roll(odd, head_size, 1)),
                    jnp.where(low, pltpu.roll(even, head_size, 1), odd),
                ],
                axis=0,
            )
        )
    attended = jnp.concatenate(pieces, axis=1)
    gated = layer_norm(attended, attn_gain_ref[...]) * gate_buf[...].astype(jnp.float32)
    mixed = tokens_ref[...].astype(jnp.float32) + jnp.dot(
        gated.astype(jnp.bfloat16), w_out_ref[...], preferred_element_type=jnp.float32
    )
    out_ref[...] = mixed.astype(jnp.bfloat16)


def solution(mesh):
    parts = mesh.shape["pb"]

    def body(tokens, stamps, norm_gain, w_proj, rel_bias, attn_gain, w_out):
        rows, width = tokens.shape
        heads = rel_bias.shape[0]
        splits = parts // heads
        slots = parts // splits
        blocks_per_tile = max(1, 384 // rows)
        vmem = pl.BlockSpec(memory_space=pltpu.VMEM)
        return pl.pallas_call(
            functools.partial(kernel, parts, heads),
            out_shape=jax.ShapeDtypeStruct((rows, width), jnp.bfloat16),
            in_specs=[pl.BlockSpec(memory_space=pltpu.HBM)] * 7,
            out_specs=vmem,
            scratch_shapes=[
                pltpu.VMEM((rows, width), jnp.bfloat16),
                pltpu.VMEM((1, rows), jnp.int32),
                pltpu.VMEM((1, width), jnp.float32),
                pltpu.VMEM(w_proj.shape, jnp.bfloat16),
                pltpu.SMEM(rel_bias.shape, jnp.float32),
                pltpu.VMEM((1, width), jnp.float32),
                pltpu.VMEM(w_out.shape, jnp.bfloat16),
                pltpu.VMEM((heads, rows, LANES), jnp.bfloat16),
                pltpu.VMEM((heads, rows // 2, LANES), jnp.bfloat16),
                pltpu.VMEM((parts, rows, LANES), jnp.bfloat16),
                pltpu.VMEM((slots, rows // 2, LANES), jnp.bfloat16),
                pltpu.VMEM((slots, rows, LANES), jnp.bfloat16),
                pltpu.VMEM((parts, 1, rows), jnp.int32),
                pltpu.VMEM((parts // blocks_per_tile, 1, blocks_per_tile * rows), jnp.int32),
                pltpu.VMEM((slots, rows, LANES), jnp.int32),
                pltpu.VMEM((slots, rows, LANES), jnp.float32),
                pltpu.VMEM((rows, width), jnp.bfloat16),
                pltpu.VMEM((slots, rows // 2, LANES), jnp.bfloat16),
                pltpu.VMEM((heads, rows // 2, LANES), jnp.bfloat16),
                pltpu.SemaphoreType.DMA((8,)),
                pltpu.SemaphoreType.DMA((heads,)),
                pltpu.SemaphoreType.DMA((heads,)),
                pltpu.SemaphoreType.DMA((slots, splits)),
                pltpu.SemaphoreType.DMA((parts,)),
                pltpu.SemaphoreType.DMA((slots,)),
                pltpu.SemaphoreType.DMA((parts,)),
                pltpu.SemaphoreType.DMA((parts,)),
                pltpu.SemaphoreType.DMA((slots,)),
                pltpu.SemaphoreType.DMA((heads,)),
            ],
            compiler_params=pltpu.CompilerParams(
                collective_id=0, has_side_effects=True
            ),
        )(
            tokens,
            stamps.reshape(1, rows),
            norm_gain.reshape(1, width),
            w_proj,
            rel_bias,
            attn_gain.reshape(1, width),
            w_out,
        )

    return jax.shard_map(
        body,
        mesh=mesh,
        in_specs=(P(("groups", "pb"), None), P(("groups", "pb")), P(), P(), P(), P(), P()),
        out_specs=P(("groups", "pb"), None),
        check_vma=False,
    )
```

```python
import functools

import jax
import jax.numpy as jnp
from jax import lax
from jax.experimental import pallas as pl
from jax.experimental.pallas import tpu as pltpu
from jax.sharding import PartitionSpec as P

EPSILON = 1e-05
LANES = 128


def layer_norm(values, gain):
    centered = values - jnp.mean(values, axis=-1, keepdims=True)
    spread = jnp.mean(centered * centered, axis=-1, keepdims=True)
    return centered * lax.rsqrt(spread + EPSILON) * gain


def kernel(
    parts,
    heads,
    tokens_hbm,
    stamps_hbm,
    norm_gain_hbm,
    w_proj_hbm,
    bias_hbm,
    attn_gain_hbm,
    w_out_hbm,
    out_ref,
    tokens_ref,
    stamps_ref,
    norm_gain_ref,
    w_proj_ref,
    bias_ref,
    attn_gain_ref,
    w_out_ref,
    kv_send,
    q_send,
    kv_all,
    q_all,
    query_buf,
    stamp_all,
    stamp_keys,
    stamp_rows,
    total_buf,
    gate_buf,
    back_buf,
    att_buf,
    load_sem,
    kv_send_sem,
    q_send_sem,
    fwd_sem,
    kv_sem,
    q_sem,
    stamp_send_sem,
    stamp_sem,
    back_sem,
    att_sem,
):
    rows, width = tokens_ref.shape
    half = rows // 2
    head_size = width // heads
    splits = parts // heads
    slots = heads
    near = slots // 2
    blocks_per_tile = max(1, 384 // rows)
    key_tile = blocks_per_tile * rows
    group_tiles = splits // blocks_per_tile
    buckets = bias_ref.shape[1]

    loads = [
        pltpu.make_async_copy(source, target, load_sem.at[index])
        for index, (source, target) in enumerate(
            [
                (tokens_hbm, tokens_ref),
                (norm_gain_hbm, norm_gain_ref),
                (w_proj_hbm.at[:, width:], w_proj_ref.at[:, width:]),
                (stamps_hbm, stamps_ref),
                (bias_hbm, bias_ref),
                (w_proj_hbm.at[:, :width], w_proj_ref.at[:, :width]),
                (attn_gain_hbm, attn_gain_ref),
                (w_out_hbm, w_out_ref),
            ]
        )
    ]
    for load in loads:
        load.start()

    me = lax.axis_index("pb")
    my_head = me // splits
    my_split = me % splits
    upper = my_head // near
    my_place = my_head % near
    near_first = upper * near
    far_first = near - near_first

    def split_of(block):
        place = block % splits
        odd = (block // splits) % 2
        return place + odd * (splits - 1 - 2 * place)

    def block_of(slot, split):
        odd = slot % 2
        return slot * splits + split + odd * (splits - 1 - 2 * split)

    def remote(source, target, send, receive, device):
        return pltpu.make_async_remote_copy(
            src_ref=source,
            dst_ref=target,
            send_sem=send,
            recv_sem=receive,
            device_id={"pb": device},
            device_id_type=pl.DeviceIdType.MESH,
        )

    barrier = pltpu.get_barrier_semaphore()

    def greet(step, carry):
        other = lax.rem(me + step, parts)
        pl.semaphore_signal(
            barrier, inc=1, device_id={"pb": other}, device_id_type=pl.DeviceIdType.MESH
        )
        return carry

    lax.fori_loop(1, parts, greet, 0)

    low = lax.broadcasted_iota(jnp.int32, (1, LANES), 1) < head_size

    for load in loads[:3]:
        load.wait()
    normed = layer_norm(tokens_ref[...].astype(jnp.float32), norm_gain_ref[...]).astype(jnp.bfloat16)
    front = jnp.dot(normed, w_proj_ref[:, width : 2 * width], preferred_element_type=jnp.float32)
    scaled = front.astype(jnp.bfloat16).astype(jnp.float32) * (0.5 * head_size ** (-0.5))
    back = jnp.dot(normed, w_proj_ref[:, 2 * width :], preferred_element_type=jnp.float32)
    for pair in range(heads // 2):
        cols = slice(pair * LANES, (pair + 1) * LANES)
        key_cols = back[:, :width][:, cols]
        value_cols = back[:, width:][:, cols]
        query_cols = scaled[:, cols]
        kv_send[2 * pair] = jnp.where(
            low, key_cols, pltpu.roll(value_cols, head_size, 1)
        ).astype(jnp.bfloat16)
        kv_send[2 * pair + 1] = jnp.where(
            low, pltpu.roll(key_cols, head_size, 1), value_cols
        ).astype(jnp.bfloat16)
        top, bottom = query_cols[:half], query_cols[half:]
        q_send[2 * pair] = jnp.where(low, top, pltpu.roll(bottom, head_size, 1)).astype(jnp.bfloat16)
        q_send[2 * pair + 1] = jnp.where(low, pltpu.roll(top, head_size, 1), bottom).astype(jnp.bfloat16)
    loads[3].wait()
    loads[4].wait()

    my_home = split_of(me)

    def stamp_copy(target):
        return remote(
            stamps_ref, stamp_all.at[me], stamp_send_sem.at[target], stamp_sem.at[me], target
        )

    def kv_copy(head, target):
        return remote(kv_send.at[head], kv_all.at[me], kv_send_sem.at[head], kv_sem.at[me], target)

    def q_copy(head, target):
        return remote(q_send.at[head], q_all.at[my_head], q_send_sem.at[head], q_sem.at[my_head], target)

    def each_head(first, act):
        def one(step, carry):
            head = first + lax.rem(my_place + step, near)
            target = head * splits + my_home

            @pl.when(target != me)
            def _():
                act(head, target)

            return carry

        lax.fori_loop(0, near, one, 0)

    def send_stamps(step, carry):
        stamp_copy(lax.rem(me + step, parts)).start()
        return carry

    def start_both(head, target):
        q_copy(head, target).start()
        kv_copy(head, target).start()

    pl.semaphore_wait(barrier, parts - 1)
    lax.fori_loop(1, parts, send_stamps, 0)
    each_head(near_first, start_both)
    each_head(far_first, lambda head, target: q_copy(head, target).start())
    each_head(far_first, lambda head, target: kv_copy(head, target).start())

    stamp_all[me] = stamps_ref[...]

    @pl.when(my_home == my_split)
    def _():
        kv_all[me] = kv_send[my_head]
        q_all[my_head] = q_send[my_head]

    loads[5].wait()
    gate_proj = jnp.dot(normed, w_proj_ref[:, :width], preferred_element_type=jnp.float32)
    gate_buf[...] = jax.nn.silu(gate_proj).astype(jnp.bfloat16)
    total_buf[...] = jnp.zeros_like(total_buf)

    zeros_count = lax.broadcasted_iota(jnp.int32, (8, LANES), 1)
    bucket = jnp.clip((33 - zeros_count) >> 1, 0, buckets - 1)
    table = jnp.zeros((8, LANES), jnp.float32)
    for bucket_id in range(buckets):
        table = jnp.where(bucket == bucket_id, 0.5 * bias_ref[my_head, bucket_id], table)
    table_two = jnp.broadcast_to(table[:1], (2 * rows, LANES))
    table = table_two[:rows]

    def wait_stamps(step, carry):
        source = lax.rem(me + step, parts)
        remote(
            stamps_ref, stamp_all.at[source], stamp_send_sem.at[source], stamp_sem.at[source], source
        ).wait_recv()
        return carry

    lax.fori_loop(1, parts, wait_stamps, 0)

    for tile in range(parts // blocks_per_tile):
        stamp_keys[tile] = jnp.concatenate(
            [stamp_all[tile * blocks_per_tile + place] for place in range(blocks_per_tile)], axis=1
        )

    def turn_stamps(slot, carry):
        block = block_of(slot, my_split)
        stamp_rows[slot] = jnp.transpose(jnp.broadcast_to(stamp_all[block], (LANES, rows)))
        return carry

    lax.fori_loop(0, slots, turn_stamps, 0)

    def forward(slot, source, step):
        peer = my_head * splits + lax.rem(my_split + step, splits)
        return remote(
            kv_all.at[source], kv_all.at[source], fwd_sem.at[slot, step], kv_sem.at[source], peer
        )

    def take_direct(slot):
        source = block_of(slot, my_split)

        @pl.when(source != me)
        def _():
            remote(
                kv_send.at[0], kv_all.at[source], kv_send_sem.at[0], kv_sem.at[source], source
            ).wait_recv()

        for step in range(1, splits):
            forward(slot, source, step).start()

    def take_forwarded(slot):
        for step in range(1, splits):
            source = block_of(slot, lax.rem(my_split + step, splits))
            forward(slot, source, step).wait_recv()

    def take_query(slot):
        source = block_of(slot, my_split)

        @pl.when(source != me)
        def _():
            remote(
                q_send.at[0], q_all.at[slot], q_send_sem.at[0], q_sem.at[slot], source
            ).wait_recv()

        packed = q_all[slot].astype(jnp.float32)
        query_buf[slot] = jnp.concatenate(
            [jnp.where(low, packed, 0.0), jnp.where(low, pltpu.roll(packed, head_size, 1), 0.0)], axis=0
        ).astype(jnp.bfloat16)

    row_id = lax.broadcasted_iota(jnp.int32, (rows, LANES), 0)
    col_id = lax.broadcasted_iota(jnp.int32, (rows, LANES), 1)

    def visit_tile(slot, block, tile, masked):
        key_value = kv_all[pl.ds(tile * blocks_per_tile, blocks_per_tile)]
        key_value = key_value.reshape(key_tile, LANES)
        scores = lax.dot_general(
            query_buf[slot], key_value, (((1,), (1,)), ((), ())), preferred_element_type=jnp.float32
        )
        query_stamp = stamp_rows[slot]
        weights = []
        for first in range(0, key_tile, LANES):
            elapsed = query_stamp - stamp_keys[tile, :, first : first + LANES]
            bias = jnp.take_along_axis(table, lax.clz(elapsed), axis=1, mode="promise_in_bounds")
            halved = scores[:, first : first + LANES] + bias
            weight = halved + halved * jnp.tanh(halved)
            if masked:
                ahead = tile * key_tile + first - block * rows
                weight = jnp.where(col_id + ahead <= row_id, weight, 0.0)
            weights.append(weight.astype(jnp.bfloat16))
        total_buf[slot] += jnp.dot(
            jnp.concatenate(weights, axis=1), key_value, preferred_element_type=jnp.float32
        )

    def visit_two(slot, group):
        def one(tile, carry):
            key_value = kv_all[pl.ds(tile * blocks_per_tile, blocks_per_tile)]
            key_value = key_value.reshape(key_tile, LANES)
            queries = query_buf[pl.ds(slot, 2)].reshape(2 * rows, LANES)
            query_stamp = stamp_rows[pl.ds(slot, 2)].reshape(2 * rows, LANES)
            scores = lax.dot_general(
                queries, key_value, (((1,), (1,)), ((), ())), preferred_element_type=jnp.float32
            )
            weights = []
            for first in range(0, key_tile, LANES):
                elapsed = query_stamp - stamp_keys[tile, :, first : first + LANES]
                bias = jnp.take_along_axis(table_two, lax.clz(elapsed), axis=1, mode="promise_in_bounds")
                halved = scores[:, first : first + LANES] + bias
                weights.append((halved + halved * jnp.tanh(halved)).astype(jnp.bfloat16))
            sums = jnp.dot(
                jnp.concatenate(weights, axis=1), key_value, preferred_element_type=jnp.float32
            )
            total_buf[pl.ds(slot, 2)] += sums.reshape(2, rows, LANES)
            return carry

        lax.fori_loop(group * group_tiles, (group + 1) * group_tiles, one, 0)

    def visit_later(first, end, group):
        count = end - first

        def two(step, carry):
            visit_two(first + 2 * step, group)
            return carry

        lax.fori_loop(0, count // 2, two, 0)

        @pl.when(count % 2 == 1)
        def _():
            visit_before(end - 1, group)

    def visit_before(slot, group):
        def one(tile, carry):
            visit_tile(slot, 0, tile, False)
            return carry

        lax.fori_loop(group * group_tiles, (group + 1) * group_tiles, one, 0)

    def visit_own(slot):
        block = block_of(slot, my_split)
        last = block // blocks_per_tile

        def one(tile, carry):
            visit_tile(slot, block, tile, False)
            return carry

        if group_tiles > 1:
            lax.fori_loop(slot * group_tiles, last, one, 0)
        visit_tile(slot, block, last, True)

    def send_back(slot, target):
        return remote(
            back_buf.at[slot], att_buf.at[my_head], back_sem.at[slot], att_sem.at[my_head], target
        )

    def finish(slot, carry):
        block = block_of(slot, my_split)
        total = total_buf[slot]
        result = jnp.where(low, pltpu.roll(total[:half], head_size, 1), total[half:]).astype(jnp.bfloat16)
        back_buf[slot] = result

        @pl.when(block == me)
        def _():
            att_buf[my_head] = result

        @pl.when(block != me)
        def _():
            send_back(slot, block).start()

        return carry

    def take_near(slot, carry):
        take_direct(slot)
        take_query(slot)
        return carry

    lax.fori_loop(near_first, near_first + near, take_near, 0)

    def near_group(group, carry):
        take_forwarded(group)
        visit_own(group)

        visit_later(group + 1, near_first + near, group)
        return carry

    lax.fori_loop(near_first, near_first + near, near_group, 0)

    lower_end = near * (1 - upper)
    lax.fori_loop(0, lower_end, finish, 0)

    def far_query(slot, carry):
        take_query(slot)
        return carry

    lax.fori_loop(far_first, far_first + near, far_query, 0)

    def later_queries(group, carry):
        visit_later(near, slots, group)
        return carry

    lax.fori_loop(0, lower_end, later_queries, 0)

    def far_at(step):
        return far_first + lax.rem(my_place - step + near, near)

    take_direct(far_at(0))

    def far_group(step, carry):
        group = far_at(step)
        take_forwarded(group)

        @pl.when(step + 1 < near)
        def _():
            take_direct(far_at(step + 1))

        visit_own(group)
        visit_later(group + 1, slots, group)
        return carry

    lax.fori_loop(0, near - 1, far_group, 0)

    last_group = far_at(near - 1)
    lax.fori_loop(lower_end, last_group, finish, 0)
    take_forwarded(last_group)
    visit_own(last_group)
    finish(last_group, 0)

    def last_one(slot, carry):
        visit_before(slot, last_group)
        return finish(slot, carry)

    lax.fori_loop(last_group + 1, slots, last_one, 0)

    def drain_both(head, target):
        q_copy(head, target).wait_send()
        kv_copy(head, target).wait_send()

    each_head(near_first, drain_both)
    each_head(far_first, drain_both)

    def drain(step, carry):
        stamp_copy(lax.rem(me + step, parts)).wait_send()
        return carry

    lax.fori_loop(1, parts, drain, 0)

    def drain_slot(slot, carry):
        source = block_of(slot, my_split)
        for step in range(1, splits):
            forward(slot, source, step).wait_send()

        @pl.when(source != me)
        def _():
            send_back(slot, source).wait_send()

        return carry

    lax.fori_loop(0, slots, drain_slot, 0)
    loads[6].wait()
    loads[7].wait()

    def take_back(step, carry):
        head = lax.rem(my_head + step, heads)
        source = head * splits + my_home

        @pl.when(source != me)
        def _():
            remote(
                back_buf.at[0], att_buf.at[head], back_sem.at[0], att_sem.at[head], source
            ).wait_recv()

        return carry

    lax.fori_loop(0, heads, take_back, 0)

    pieces = []
    for pair in range(heads // 2):
        even = att_buf[2 * pair].astype(jnp.float32)
        odd = att_buf[2 * pair + 1].astype(jnp.float32)
        pieces.append(
            jnp.concatenate(
                [
                    jnp.where(low, even, pltpu.roll(odd, head_size, 1)),
                    jnp.where(low, pltpu.roll(even, head_size, 1), odd),
                ],
                axis=0,
            )
        )
    attended = jnp.concatenate(pieces, axis=1)
    gated = layer_norm(attended, attn_gain_ref[...]) * gate_buf[...].astype(jnp.float32)
    mixed = tokens_ref[...].astype(jnp.float32) + jnp.dot(
        gated.astype(jnp.bfloat16), w_out_ref[...], preferred_element_type=jnp.float32
    )
    out_ref[...] = mixed.astype(jnp.bfloat16)


def solution(mesh):
    parts = mesh.shape["pb"]

    def body(tokens, stamps, norm_gain, w_proj, rel_bias, attn_gain, w_out):
        rows, width = tokens.shape
        heads = rel_bias.shape[0]
        splits = parts // heads
        slots = parts // splits
        blocks_per_tile = max(1, 384 // rows)
        vmem = pl.BlockSpec(memory_space=pltpu.VMEM)
        return pl.pallas_call(
            functools.partial(kernel, parts, heads),
            out_shape=jax.ShapeDtypeStruct((rows, width), jnp.bfloat16),
            in_specs=[pl.BlockSpec(memory_space=pltpu.HBM)] * 7,
            out_specs=vmem,
            scratch_shapes=[
                pltpu.VMEM((rows, width), jnp.bfloat16),
                pltpu.VMEM((1, rows), jnp.int32),
                pltpu.VMEM((1, width), jnp.float32),
                pltpu.VMEM(w_proj.shape, jnp.bfloat16),
                pltpu.SMEM(rel_bias.shape, jnp.float32),
                pltpu.VMEM((1, width), jnp.float32),
                pltpu.VMEM(w_out.shape, jnp.bfloat16),
                pltpu.VMEM((heads, rows, LANES), jnp.bfloat16),
                pltpu.VMEM((heads, rows // 2, LANES), jnp.bfloat16),
                pltpu.VMEM((parts, rows, LANES), jnp.bfloat16),
                pltpu.VMEM((slots, rows // 2, LANES), jnp.bfloat16),
                pltpu.VMEM((slots, rows, LANES), jnp.bfloat16),
                pltpu.VMEM((parts, 1, rows), jnp.int32),
                pltpu.VMEM((parts // blocks_per_tile, 1, blocks_per_tile * rows), jnp.int32),
                pltpu.VMEM((slots, rows, LANES), jnp.int32),
                pltpu.VMEM((slots, rows, LANES), jnp.float32),
                pltpu.VMEM((rows, width), jnp.bfloat16),
                pltpu.VMEM((slots, rows // 2, LANES), jnp.bfloat16),
                pltpu.VMEM((heads, rows // 2, LANES), jnp.bfloat16),
                pltpu.SemaphoreType.DMA((8,)),
                pltpu.SemaphoreType.DMA((heads,)),
                pltpu.SemaphoreType.DMA((heads,)),
                pltpu.SemaphoreType.DMA((slots, splits)),
                pltpu.SemaphoreType.DMA((parts,)),
                pltpu.SemaphoreType.DMA((slots,)),
                pltpu.SemaphoreType.DMA((parts,)),
                pltpu.SemaphoreType.DMA((parts,)),
                pltpu.SemaphoreType.DMA((slots,)),
                pltpu.SemaphoreType.DMA((heads,)),
            ],
            compiler_params=pltpu.CompilerParams(
                collective_id=0, has_side_effects=True
            ),
        )(
            tokens,
            stamps.reshape(1, rows),
            norm_gain.reshape(1, width),
            w_proj,
            rel_bias,
            attn_gain.reshape(1, width),
            w_out,
        )

    return jax.shard_map(
        body,
        mesh=mesh,
        in_specs=(P(("groups", "pb"), None), P(("groups", "pb")), P(), P(), P(), P(), P()),
        out_specs=P(("groups", "pb"), None),
        check_vma=False,
    )
```
